32 devices in a mesh: seq: 16 (over z, x, core), fsdp: 2 (over y).
Axes of the slice: x: 2, y: 2, z: 4, core: 2. Of those that a mesh axis runs over, the one named last changes fastest.
Arguments:
- hidden_next: bfloat16 [4096, 8192], P('seq'), may hold values from -6 to 6
- values_next: bfloat16 [4096, 8192], P('seq', 'fsdp'), may hold values from -6 to 6
- seg_next: int32 [4], replicated, may hold values from 1 to 2048, 4096 in all
- proj_bc: bfloat16 [8192, 1024], P(('seq', 'fsdp')), may hold values from -0.046875 to 0.046875
- proj_dt: bfloat16 [8192, 128], P(('seq', 'fsdp')), may hold values from -0.0625 to 0.0625
- dt_bias: float32 [128], replicated, may hold values from -4 to -2.5
- decay_rate: float32 [128], replicated, may hold values from 0 to 1, as said below
- skip_gain: float32 [128], replicated, may hold values from 0.5 to 1.5
- bc_prev: bfloat16 [4096, 1024], P('seq'), may hold values from -4 to 4
- dt_prev: float32 [4096, 128], P('seq', 'fsdp'), may hold values from 0.01 to 0.3
- seg_prev: int32 [4], replicated, may hold values from 1 to 2048, 4096 in all
- grad_prev: bfloat16 [4096, 8192], P('seq', 'fsdp'), may hold values from -6 to 6
Outputs:
- out_next: bfloat16 [4096, 8192], P('seq', 'fsdp')
- grad_values: bfloat16 [4096, 8192], P('seq', 'fsdp')
The draws below stay inside these ranges and needn't reach their ends.
Inputs may be any that keep to these rules, and one draw needn't show every extreme that they name: `seg_next`: lengths of the rollout's 4 segments in order, summing to 4096. `seg_prev`: lengths of the rollout's 4 segments in order, summing to 4096. `decay_rate`: positive.
All inputs are finite; a program needn't handle non-finite values.
Results may differ from the reference program's by a relative error of at most 0.0064.
Values may be sent and summed in bfloat16 or wider, within the bound.
A program may use at most 192 MiB of HBM per device.

```python
import math
import jax
import jax.numpy as jnp
import numpy as np
from jax import lax

D = 8192
HW = 128
P_SIZE = 64
GW = 4
N = 128
SPAN = 128
NSEG = 4
SEQ_LEN = 4096
BCW = 1024


def draw_decay_rate(key, part):
    streams = jax.random.split(jax.random.fold_in(key, 11), 3)
    lasting = jax.random.uniform(streams[0], (HW,)) < 0.5
    slow_rate = jnp.exp(jax.random.uniform(streams[1], (HW,), minval=jnp.log(5.0), maxval=jnp.log(20.0))) / SEQ_LEN
    fast_rate = jnp.exp(jax.random.uniform(streams[2], (HW,), minval=jnp.log(0.25), maxval=jnp.log(0.8)))
    return jnp.where(lasting, slow_rate, fast_rate).astype(jnp.float32)


def spiked(values, stream_key, source, target, blocks, factor):
    owner, partner = [(jnp.arange(values.shape[position]) // (values.shape[position] // blocks)).reshape([-1 if axis == position else 1 for axis in range(values.ndim)]) for position in (source, target)]
    chosen = jax.random.permutation(stream_key, blocks)[partner]
    strong = (owner == chosen) | (owner == (partner + blocks // 2) % blocks)
    return jnp.where(strong, factor * values, values)


def block_scale(rng, shape, cuts, least, largest):
    def one(axis_at, shards_of):
        heights = jax.random.uniform(jax.random.fold_in(jax.random.fold_in(rng, 6), axis_at), (shards_of,), jnp.float32, least / len(cuts), largest / len(cuts))
        return jnp.repeat(jnp.exp(heights), shape[axis_at] // shards_of).reshape((-1,) + (1,) * (len(shape) - axis_at - 1))

    factor_of = one(*cuts[0])
    for cut in cuts[1:]:
        factor_of = factor_of * one(*cut)
    return factor_of


def split_up(amount, total, reach, lean):
    loads = [(1 << 20) // math.isqrt(rank ** lean) + 1 for rank in range(2, amount + 1)]
    rest, counts = total - reach - (amount - 1), [1] * (amount - 1)
    while rest > 0:
        free = [i for i in range(amount - 1) if counts[i] < reach]
        pool, left = sum([loads[i] for i in free]), rest
        for i in free:
            extra = min(reach - counts[i], max(1, left * loads[i] // pool), rest)
            counts[i] = counts[i] + extra
            rest = rest - extra
    return np.array([reach] + counts)


def uneven(stream_key, count, total, limit, slope):
    if count == 2:
        one = jax.random.randint(stream_key, (), max(1, total - limit), min(limit, total - 1) + 1)
        return jnp.stack([one, total - one])
    sizes = jnp.asarray(split_up(count, total, limit, slope), jnp.int32)
    pairs = (count - 1) // 2
    donor, sink = sizes[1:1 + 2 * pairs:2], sizes[2:2 + 2 * pairs:2]
    slack = jnp.minimum(donor - 1, limit - sink)
    shifted = jax.random.randint(jax.random.fold_in(stream_key, 1), (pairs,), 0, 1 << 20) % (slack + 1)
    sizes = sizes.at[1:1 + 2 * pairs:2].set(donor - shifted).at[2:2 + 2 * pairs:2].set(sink + shifted)
    return sizes[jax.random.permutation(jax.random.fold_in(stream_key, 2), count)]


def noise(own_key, shape, scale, most, pieces=(), kind=jnp.bfloat16):
    factor_of = block_scale(own_key, shape, pieces, -0.22, 0.18) if pieces else 1.0
    drawn = jax.random.normal(own_key, shape, jnp.float32) * scale * factor_of
    return jnp.minimum(jnp.maximum(drawn, -most), most).astype(kind)


def bell_draw_with(stream_key, extent, width, most, cuts, heavy, held_as=jnp.bfloat16):
    entries = width * jax.random.normal(stream_key, extent, jnp.float32)
    if cuts:
        entries = entries * block_scale(stream_key, extent, cuts, -0.22, 0.18)
    return jnp.clip(spiked(entries, jax.random.fold_in(stream_key, 3), *heavy), -most, most).astype(held_as)


def setup_inputs(seed: int = 0) -> dict:
    splits = jax.random.split(jax.random.key(seed), 13)
    hidden_next = noise(splits[0], (SEQ_LEN, D), 1.0, 6.0, ((0, 16),))
    values_next = noise(splits[1], (SEQ_LEN, HW * P_SIZE), 1.0, 6.0, ((0, 16), (1, 2)))
    seg_next = uneven(splits[2], NSEG, SEQ_LEN, SEQ_LEN // 2, 2).astype(jnp.int32)
    proj_bc = bell_draw_with(splits[3], (D, BCW), (D * 8) ** -0.5, 0.046875, ((0, 32),), (0, 1, 32, 2.75))
    proj_dt = noise(splits[4], (D, HW), D ** -0.5, 0.0625, ((0, 32),))
    dt_bias = jnp.clip(jax.random.uniform(splits[5], (HW,), jnp.float32, -4.0, -2.5), -4.0, -2.5)
    decay_rate = draw_decay_rate(jax.random.fold_in(splits[12], 71), 0)
    skip_gain = jnp.clip(jax.random.uniform(splits[7], (HW,), jnp.float32, 0.5, 1.5), 0.5, 1.5)
    bc_prev = noise(splits[8], (SEQ_LEN, BCW), 0.3, 4.0, ((0, 16),))
    dt_prev = jnp.clip(jnp.exp(math.log(0.3) - 3.4011974 * jax.random.uniform(splits[9], (SEQ_LEN, HW), jnp.float32) ** block_scale(splits[9], (SEQ_LEN, HW), ((0, 16), (1, 2)), -0.2, 0.2)), 0.01, 0.3)
    seg_prev = uneven(splits[10], NSEG, SEQ_LEN, SEQ_LEN // 2, 2).astype(jnp.int32)
    grad_prev = noise(splits[11], (SEQ_LEN, HW * P_SIZE), 1.0, 6.0, ((0, 16), (1, 2)))
    return dict(hidden_next=hidden_next, values_next=values_next, seg_next=seg_next, proj_bc=proj_bc, proj_dt=proj_dt, dt_bias=dt_bias, decay_rate=decay_rate, skip_gain=skip_gain, bc_prev=bc_prev, dt_prev=dt_prev, seg_prev=seg_prev, grad_prev=grad_prev)


def segment_table(lengths, tokens_total):
    bounds = jnp.cumsum(lengths)[:-1].astype(jnp.int32)
    places = jnp.arange(tokens_total + 1, dtype=jnp.int32) - 1
    return jnp.sum((bounds[None, :] <= places[:, None]).astype(jnp.int32), axis=1)


def block_parts(bc_block, dt_block, seg_ext, decay_rate):
    span_len = bc_block.shape[0]
    half_cols = bc_block.shape[1] // 2
    b_vectors = bc_block[:, :half_cols].reshape(span_len, GW, N)
    c_vectors = bc_block[:, half_cols:].reshape(span_len, GW, N)
    before = seg_ext[0]
    segment = seg_ext[1:]
    cumulative = jnp.cumsum(-dt_block * decay_rate[None, :], axis=0)
    final_cum = cumulative[-1]
    places = jnp.arange(span_len)
    linked = (segment[:, None] == segment[None, :]) & (places[:, None] >= places[None, :])
    scores = jnp.einsum("tgn,sgn->gts", c_vectors.astype(jnp.float32), b_vectors.astype(jnp.float32),
                        precision=lax.Precision.HIGHEST)
    by_head = cumulative.T
    spread = by_head[:, :, None] - by_head[:, None, :]
    decays = jnp.exp(jnp.where(linked[None], spread, -jnp.inf))
    weighted = (decays * dt_block.T[:, None, :]).reshape(GW, HW // GW, span_len, span_len)
    mixing = (weighted * scores[:, None]).reshape(HW, span_len, span_len).astype(jnp.bfloat16)
    keep_final = (segment == segment[-1]).astype(jnp.float32)
    linked_in = (segment == before).astype(jnp.float32)
    send_factor = keep_final[:, None] * jnp.exp(final_cum[None, :] - cumulative) * dt_block
    read_factor = linked_in[:, None] * jnp.exp(cumulative)
    carry_decay = (segment[-1] == before).astype(jnp.float32) * jnp.exp(final_cum)
    return b_vectors, c_vectors, mixing, send_factor, read_factor, carry_decay


def outer_sum(values, vectors):
    span_len, heads_all, head_dim = values.shape
    grouped = values.reshape(span_len, GW, heads_all // GW, head_dim).astype(jnp.float32)
    result = jnp.einsum("sgqp,sgn->gqpn", grouped, vectors.astype(jnp.float32), precision=lax.Precision.HIGHEST)
    return result.reshape(heads_all, head_dim, vectors.shape[2])


def read_state(state_now, vectors, factor):
    heads_all, head_dim, state_dim = state_now.shape
    grouped = state_now.reshape(GW, heads_all // GW, head_dim, state_dim)
    result = jnp.einsum("gqpn,tgn->tgqp", grouped, vectors.astype(jnp.float32), precision=lax.Precision.HIGHEST)
    return result.reshape(vectors.shape[0], heads_all, head_dim) * factor[:, :, None]


def forward_rollout(hidden, inputs, lengths, proj_bc, proj_dt, dt_bias, decay_rate, skip_gain):
    dt_all = jax.nn.softplus(jnp.dot(hidden, proj_dt, preferred_element_type=jnp.float32) + dt_bias[None, :])
    bc_all = jnp.dot(hidden, proj_bc, preferred_element_type=jnp.float32).astype(jnp.bfloat16)
    seg_all = segment_table(lengths, SEQ_LEN)

    def advance(state_now, block_id):
        offset = (block_id * SPAN).astype(jnp.int32)
        bc_block = lax.dynamic_slice_in_dim(bc_all, offset, SPAN, 0)
        dt_block = lax.dynamic_slice_in_dim(dt_all, offset, SPAN, 0)
        seg_ext = lax.dynamic_slice_in_dim(seg_all, offset, SPAN + 1, 0)
        values = lax.dynamic_slice_in_dim(inputs, offset, SPAN, 0).reshape(SPAN, HW, P_SIZE)
        b_vectors, c_vectors, mixing, send_factor, read_factor, carry_decay = block_parts(
            bc_block, dt_block, seg_ext, decay_rate)
        inside = jnp.einsum("hts,shp->thp", mixing.astype(jnp.float32), values.astype(jnp.float32),
                            precision=lax.Precision.HIGHEST)
        output = inside + read_state(state_now, c_vectors, read_factor) + skip_gain[None, :, None] * values.astype(jnp.float32)
        scaled = (values.astype(jnp.float32) * send_factor[:, :, None]).astype(jnp.bfloat16)
        state_next = carry_decay[:, None, None] * state_now + outer_sum(scaled, b_vectors)
        return state_next, output.astype(jnp.bfloat16).reshape(SPAN, HW * P_SIZE)

    blocks_all = jnp.arange(SEQ_LEN // SPAN, dtype=jnp.int32)
    _, outputs = lax.scan(advance, jnp.zeros((HW, P_SIZE, N), jnp.float32), blocks_all)
    return outputs.reshape(SEQ_LEN, HW * P_SIZE)


def backward_rollout(bc_all, dt_all, lengths, grads_all, decay_rate, skip_gain):
    seg_all = segment_table(lengths, SEQ_LEN)

    def retreat(state_now, block_id):
        offset = (block_id * SPAN).astype(jnp.int32)
        bc_block = lax.dynamic_slice_in_dim(bc_all, offset, SPAN, 0)
        dt_block = lax.dynamic_slice_in_dim(dt_all, offset, SPAN, 0)
        seg_ext = lax.dynamic_slice_in_dim(seg_all, offset, SPAN + 1, 0)
        grad_block = lax.dynamic_slice_in_dim(grads_all, offset, SPAN, 0).reshape(SPAN, HW, P_SIZE)
        b_vectors, c_vectors, mixing, send_factor, read_factor, carry_decay = block_parts(
            bc_block, dt_block, seg_ext, decay_rate)
        inside = jnp.einsum("hts,thp->shp", mixing.astype(jnp.float32), grad_block.astype(jnp.float32),
                            precision=lax.Precision.HIGHEST)
        output = inside + read_state(state_now, b_vectors, send_factor) + skip_gain[None, :, None] * grad_block.astype(jnp.float32)
        scaled = (grad_block.astype(jnp.float32) * read_factor[:, :, None]).astype(jnp.bfloat16)
        state_next = carry_decay[:, None, None] * state_now + outer_sum(scaled, c_vectors)
        return state_next, output.astype(jnp.bfloat16).reshape(SPAN, HW * P_SIZE)

    blocks_all = jnp.arange(SEQ_LEN // SPAN, dtype=jnp.int32)
    _, outputs = lax.scan(retreat, jnp.zeros((HW, P_SIZE, N), jnp.float32), blocks_all, reverse=True)
    return outputs.reshape(SEQ_LEN, HW * P_SIZE)


def reference(hidden_next, values_next, seg_next, proj_bc, proj_dt, dt_bias, decay_rate, skip_gain,
              bc_prev, dt_prev, seg_prev, grad_prev):
    out_next = forward_rollout(hidden_next, values_next, seg_next, proj_bc, proj_dt, dt_bias, decay_rate, skip_gain)
    grad_values = backward_rollout(bc_prev, dt_prev, seg_prev, grad_prev, decay_rate, skip_gain)
    return out_next, grad_values
```

```python
import functools

import jax
import jax.numpy as jnp
from jax import lax
from jax.experimental import pallas as pl
from jax.experimental.pallas import tpu as pltpu
from jax.sharding import PartitionSpec as P

GW = 4
SPAN = 128
LANES = 128
MESH = pl.DeviceIdType.MESH


def scan_kernel(
    back, count, nblocks, heads, groups, head_dim,
    len_ref, x_ref, p_ref, q_ref, dt_ref, decay_ref, skip_ref,
    out_ref,
    cum_s, cum_t, dt_t, fin_s, fout_s, fexp, inside, pre, keep, inbox, outbox, send_sem, recv_sem,
):
    me = lax.axis_index("seq")
    place = count - 1 - me if back else me
    nxt = me - 1 if back else me + 1
    prv = me + 1 if back else me - 1
    npair = heads * head_dim // LANES
    per = LANES // head_dim
    pair_group = npair // groups
    first, last = place == 0, place == count - 1

    barrier = pltpu.get_barrier_semaphore()

    @pl.when(jnp.logical_not(first))
    def _():
        pl.semaphore_signal(barrier, inc=1, device_id={"seq": prv}, device_id_type=MESH)

    @pl.when(jnp.logical_not(last))
    def _():
        pl.semaphore_signal(barrier, inc=1, device_id={"seq": nxt}, device_id_type=MESH)

    bound = []
    total = jnp.int32(0)
    for k in range(3):
        total = total + len_ref[k]
        bound.append(total)

    def seg_of(pos):
        s = jnp.zeros_like(pos)
        for b in bound:
            s = s + (b <= pos).astype(jnp.int32)
        return s

    slab = me * (nblocks * SPAN)
    dim0 = lax.broadcasted_iota(jnp.int32, (SPAN, SPAN), 0)
    dim1 = lax.broadcasted_iota(jnp.int32, (SPAN, SPAN), 1)
    lane = lax.broadcasted_iota(jnp.int32, (1, LANES), 1)
    tril = (dim0 >= dim1).astype(jnp.float32)

    def widen(a, c):
        res = a[:, c * per:c * per + 1]
        for k in range(1, per):
            res = jnp.where(lane >= k * head_dim, a[:, c * per + k:c * per + k + 1], res)
        return jnp.broadcast_to(res, (a.shape[0], LANES))

    for c in range(npair):
        pre[0, c] = jnp.zeros((LANES, LANES), jnp.float32)
        keep[0, c] = jnp.ones((1, LANES), jnp.float32)

    for step in range(nblocks):
        b = nblocks - 1 - step if back else step
        rows = slice(b * SPAN, (b + 1) * SPAN)
        dt = dt_ref[rows, :]
        cum = jnp.dot(tril, -(dt * decay_ref[...]), precision=lax.Precision.HIGHEST,
                      preferred_element_type=jnp.float32)
        end = cum[SPAN - 1:SPAN, :]
        cum_s[rows, :] = cum
        cum_t[b] = cum.T
        dt_t[b] = dt.T
        pos = slab + b * SPAN + lax.broadcasted_iota(jnp.int32, (SPAN, heads), 0)
        seg = seg_of(pos)
        edge = slab + b * SPAN + lax.broadcasted_iota(jnp.int32, (1, heads), 0) * 0
        seg_e = seg_of(edge + (SPAN - 1))
        seg_b = jnp.where(edge == 0, 0, seg_of(edge - 1))
        send = jnp.where(seg == seg_e, jnp.exp(end - cum), 0.0)
        read = jnp.where(seg == seg_b, jnp.exp(cum), 0.0)
        carry = jnp.where(seg_e == seg_b, jnp.exp(end), 0.0)
        f_in = read if back else send * dt
        fin_s[rows, :] = f_in
        fout_s[rows, :] = send * dt if back else read
        qt = [q_ref[rows, g * LANES:(g + 1) * LANES].T for g in range(groups)]
        for c in range(npair):
            cols = slice(c * LANES, (c + 1) * LANES)
            sent = (x_ref[rows, cols].astype(jnp.float32) * widen(f_in, c)).astype(jnp.bfloat16)
            loc = jnp.dot(qt[c // pair_group], sent, preferred_element_type=jnp.float32)
            wide = widen(carry, c)
            pre[step + 1, c] = wide * pre[step, c] + loc
            keep[step + 1, c] = wide * keep[step, c]

    def in_block():
        def one(b, _):
            start = pl.multiple_of(b * SPAN, SPAN)
            rows = pl.ds(start, SPAN)
            seg_i = seg_of(slab + start + dim0)
            seg_j = seg_of(slab + start + dim1)
            order = (dim1 >= dim0) if back else (dim1 <= dim0)
            bias = jnp.where((seg_i == seg_j) & order, 0.0, -jnp.inf)
            cum = cum_s[rows, :]
            dt = dt_ref[rows, :]
            f_out = fout_s[rows, :]
            for g in range(groups):
                gl = slice(g * LANES, (g + 1) * LANES)
                score = lax.dot_general(p_ref[rows, gl], q_ref[rows, gl], (((1,), (1,)), ((), ())),
                                        preferred_element_type=jnp.float32)
                for c in range(g * pair_group, (g + 1) * pair_group):
                    cols = slice(c * LANES, (c + 1) * LANES)
                    x = x_ref[rows, cols]
                    mixes, parts = [], []
                    for k in range(per):
                        h = c * per + k
                        col = cum[:, h:h + 1]
                        row = cum_t[b, h:h + 1, :]
                        spread = (row - col) if back else (col - row)
                        w = jnp.exp(spread + bias) * score
                        if not back:
                            w = w * dt_t[b, h:h + 1, :]
                        mixes.append(w.astype(jnp.bfloat16))
                        mine = (lane >= k * head_dim) & (lane < (k + 1) * head_dim)
                        parts.append(jnp.where(mine, x, jnp.zeros_like(x)))
                    acc = jnp.dot(jnp.concatenate(mixes, 1), jnp.concatenate(parts, 0),
                                  preferred_element_type=jnp.float32)
                    if back:
                        acc = acc * widen(dt, c)
                    inside[c, rows, :] = acc + widen(skip_ref[...], c) * x.astype(jnp.float32)
                    fexp[c, rows, :] = widen(f_out, c)
            return 0

        lax.fori_loop(0, nblocks, one, 0)

    def finish(c, state):
        g = c // pair_group
        cols = pl.ds(pl.multiple_of(c * LANES, LANES), LANES)
        gl = pl.ds(pl.multiple_of(g * LANES, LANES), LANES)
        for step in range(nblocks):
            b = nblocks - 1 - step if back else step
            rows = slice(b * SPAN, (b + 1) * SPAN)
            entering = (keep[step, c] * state + pre[step, c]).astype(jnp.bfloat16)
            y = jnp.dot(p_ref[rows, gl], entering, preferred_element_type=jnp.float32)
            out_ref[rows, cols] = (inside[c, rows, :] + fexp[c, rows, :] * y).astype(jnp.bfloat16)

    def hop(c):
        return pltpu.make_async_remote_copy(
            src_ref=outbox.at[c], dst_ref=inbox.at[c], send_sem=send_sem.at[c],
            recv_sem=recv_sem.at[c], device_id={"seq": nxt}, device_id_type=MESH)

    late = place >= 5

    @pl.when(first)
    def _():
        inbox[...] = jnp.zeros_like(inbox)

    pl.semaphore_wait(barrier, jnp.where(first, 0, 1) + jnp.where(last, 0, 1))

    def relay(c, _):
        @pl.when(jnp.logical_not(first))
        def _():
            hop(c).wait_recv()

        state = inbox[c].astype(jnp.float32)

        @pl.when(jnp.logical_not(last))
        def _():
            outbox[c] = (keep[nblocks, c] * state + pre[nblocks, c]).astype(jnp.bfloat16)
            hop(c).start()

        @pl.when(late)
        def _():
            finish(c, state)

        return 0

    def phase(ph, _):
        @pl.when(ph == jnp.where(late, 0, 1))
        def _():
            in_block()

        @pl.when(ph == 0)
        def _():
            lax.fori_loop(0, npair, relay, 0)

        return 0

    lax.fori_loop(0, 2, phase, 0)

    @pl.when(jnp.logical_not(late))
    def _():
        def one(c, _):
            finish(c, inbox[c].astype(jnp.float32))
            return 0

        lax.fori_loop(0, npair, one, 0)

    @pl.when(jnp.logical_not(last))
    def _():
        def one(c, _):
            hop(c).wait_send()
            return 0

        lax.fori_loop(0, npair, one, 0)


def scan_pass(back, lengths, x, p_vec, q_vec, dt, decay, skip):
    tokens, width = x.shape
    heads = dt.shape[1]
    groups = p_vec.shape[1] // LANES
    head_dim = width // heads
    nblocks = tokens // SPAN
    npair = width // LANES
    count = lax.axis_size("seq")
    vm = pl.BlockSpec(memory_space=pltpu.VMEM)
    f32, bf16 = jnp.float32, jnp.bfloat16
    return pl.pallas_call(
        functools.partial(scan_kernel, back, count, nblocks, heads, groups, head_dim),
        out_shape=jax.ShapeDtypeStruct((tokens, width), bf16),
        in_specs=[pl.BlockSpec(memory_space=pltpu.SMEM)] + [vm] * 6,
        out_specs=vm,
        scratch_shapes=[
            pltpu.VMEM((tokens, heads), f32),
            pltpu.VMEM((nblocks, heads, SPAN), f32),
            pltpu.VMEM((nblocks, heads, SPAN), f32),
            pltpu.VMEM((tokens, heads), f32),
            pltpu.VMEM((tokens, heads), f32),
            pltpu.VMEM((npair, tokens, LANES), f32),
            pltpu.VMEM((npair, tokens, LANES), f32),
            pltpu.VMEM((nblocks + 1, npair, LANES, LANES), f32),
            pltpu.VMEM((nblocks + 1, npair, 1, LANES), f32),
            pltpu.VMEM((npair, LANES, LANES), bf16),
            pltpu.VMEM((npair, LANES, LANES), bf16),
            pltpu.SemaphoreType.DMA((npair,)),
            pltpu.SemaphoreType.DMA((npair,)),
        ],
        compiler_params=pltpu.CompilerParams(
            collective_id=1 if back else 0, has_side_effects=True,
            vmem_limit_bytes=40 * 1024 * 1024),
        cost_estimate=pl.CostEstimate(
            flops=40_000_000_000, bytes_accessed=8 * tokens * width, transcendentals=0),
        name="back_pass" if back else "next_pass",
    )(lengths, x, p_vec, q_vec, dt, decay, skip)


def body(
    hidden_next, values_next, seg_next, proj_bc, proj_dt, dt_bias, decay_rate, skip_gain,
    bc_prev, dt_prev, seg_prev, grad_prev,
):
    tokens_dev = hidden_next.shape[0]
    bc_width = proj_bc.shape[1]
    heads_all = proj_dt.shape[1]
    fsdp_count = lax.axis_size("fsdp")
    fsdp_place = lax.axis_index("fsdp")
    seq_count = lax.axis_size("seq")
    heads_dev = heads_all // fsdp_count
    state_dim = bc_width // (2 * GW)
    per_group = heads_all // GW
    groups_dev = max(1, heads_dev // per_group)
    first_head = fsdp_place * heads_dev
    first_group = first_head // per_group
    rows_dev = proj_bc.shape[0]
    half = bc_width // 2
    gw = groups_dev * state_dim

    pieces = []
    for f in range(fsdp_count):
        g0 = (f * heads_dev // per_group) * state_dim
        pieces += [proj_bc[:, g0:g0 + gw], proj_bc[:, half + g0:half + g0 + gw],
                   proj_dt[:, f * heads_dev:(f + 1) * heads_dev]]
    cols = 2 * gw + heads_dev
    weights = lax.all_gather(jnp.concatenate(pieces, axis=1), "seq", axis=0, tiled=True)

    decay = lax.dynamic_slice_in_dim(decay_rate, first_head, heads_dev, 0)[None]
    skip = lax.dynamic_slice_in_dim(skip_gain, first_head, heads_dev, 0)[None]
    bias = lax.dynamic_slice_in_dim(dt_bias, first_head, heads_dev, 0)[None]

    b_prev = lax.dynamic_slice_in_dim(bc_prev, first_group * state_dim, gw, 1)
    c_prev = lax.dynamic_slice_in_dim(bc_prev, half + first_group * state_dim, gw, 1)
    grad_values = scan_pass(True, seg_prev, grad_prev, b_prev, c_prev, dt_prev, decay, skip)

    owned = lax.dynamic_slice_in_dim(
        hidden_next.reshape(tokens_dev, seq_count, fsdp_count, rows_dev), fsdp_place, 1, 2
    ).reshape(tokens_dev, seq_count * rows_dev)
    owned, grad_values = lax.optimization_barrier((owned, grad_values))
    if fsdp_count == 2:
        other = lax.dynamic_slice_in_dim(weights, (1 - fsdp_place) * cols, cols, 1)
        mine = lax.dynamic_slice_in_dim(weights, fsdp_place * cols, cols, 1)
        away = lax.ppermute(jnp.dot(owned, other, preferred_element_type=jnp.float32),
                            "fsdp", [(0, 1), (1, 0)])
        sums = jnp.dot(owned, mine, preferred_element_type=jnp.float32) + away
    else:
        sums = lax.psum_scatter(jnp.dot(owned, weights, preferred_element_type=jnp.float32),
                                "fsdp", scatter_dimension=1, tiled=True)
    b_next = sums[:, :gw].astype(jnp.bfloat16)
    c_next = sums[:, gw:2 * gw].astype(jnp.bfloat16)
    dt_next = jax.nn.softplus(sums[:, 2 * gw:] + bias)
    out_next = scan_pass(False, seg_next, values_next, c_next, b_next, dt_next, decay, skip)
    return (out_next, grad_values)


def solution(mesh):
    in_specs = (
        P("seq", None), P("seq", "fsdp"), P(), P(("seq", "fsdp"), None), P(("seq", "fsdp"), None),
        P(), P(), P(), P("seq", None), P("seq", "fsdp"), P(), P("seq", "fsdp"),
    )
    out_specs = (P("seq", "fsdp"), P("seq", "fsdp"))
    return jax.shard_map(body, mesh=mesh, in_specs=in_specs, out_specs=out_specs, check_vma=False)
```

```python
import functools

import jax
import jax.numpy as jnp
from jax import lax
from jax.experimental import pallas as pl
from jax.experimental.pallas import tpu as pltpu
from jax.sharding import PartitionSpec as P

GW = 4
SPAN = 128
LANES = 128
MESH = pl.DeviceIdType.MESH


def widen(a, c, head_dim):
    per = LANES // head_dim
    lane = lax.broadcasted_iota(jnp.int32, (1, LANES), 1)
    res = a[:, c * per:c * per + 1]
    for k in range(1, per):
        res = jnp.where(lane >= k * head_dim, a[:, c * per + k:c * per + k + 1], res)
    return jnp.broadcast_to(res, (a.shape[0], LANES))


def seg_maker(len_ref):
    bound = []
    total = jnp.int32(0)
    for k in range(len_ref.shape[0] - 1):
        total = total + len_ref[k]
        bound.append(total)

    def seg_of(pos):
        s = jnp.zeros_like(pos)
        for b in bound:
            s = s + (b <= pos).astype(jnp.int32)
        return s

    return seg_of


def local_states(back, dims, len_ref, x_ref, q_ref, dt_ref, decay_ref, work, pre, keep):
    nblocks, heads, groups, head_dim = dims
    cum_s, cum_t, dt_t, fout_s = work
    npair = heads * head_dim // LANES
    pair_group = npair // groups
    seg_of = seg_maker(len_ref)
    slab = lax.axis_index("seq") * (nblocks * SPAN)
    dim0 = lax.broadcasted_iota(jnp.int32, (SPAN, SPAN), 0)
    dim1 = lax.broadcasted_iota(jnp.int32, (SPAN, SPAN), 1)
    tril = (dim0 >= dim1).astype(jnp.float32)
    for c in range(npair):
        pre[0, c] = jnp.zeros((LANES, LANES), jnp.float32)
        keep[0, c] = jnp.ones((1, LANES), jnp.float32)
    for step in range(nblocks):
        b = nblocks - 1 - step if back else step
        rows = slice(b * SPAN, (b + 1) * SPAN)
        dt = dt_ref[rows, :]
        cum = jnp.dot(tril, -(dt * decay_ref[...]), precision=lax.Precision.HIGHEST,
                      preferred_element_type=jnp.float32)
        end = cum[SPAN - 1:SPAN, :]
        cum_s[rows, :] = cum
        cum_t[b] = cum.T
        dt_t[b] = dt.T
        seg = seg_of(slab + b * SPAN + lax.broadcasted_iota(jnp.int32, (SPAN, heads), 0))
        edge = slab + b * SPAN + lax.broadcasted_iota(jnp.int32, (1, heads), 0) * 0
        seg_e = seg_of(edge + (SPAN - 1))
        seg_b = jnp.where(edge == 0, 0, seg_of(edge - 1))
        send = jnp.where(seg == seg_e, jnp.exp(end - cum), 0.0) * dt
        read = jnp.where(seg == seg_b, jnp.exp(cum), 0.0)
        carry = jnp.where(seg_e == seg_b, jnp.exp(end), 0.0)
        f_in = read if back else send
        fout_s[rows, :] = send if back else read
        qt = [q_ref[rows, g * LANES:(g + 1) * LANES].T for g in range(groups)]
        for c in range(npair):
            cols = slice(c * LANES, (c + 1) * LANES)
            sent = (x_ref[rows, cols].astype(jnp.float32) * widen(f_in, c, head_dim)).astype(jnp.bfloat16)
            loc = jnp.dot(qt[c // pair_group], sent, preferred_element_type=jnp.float32)
            wide = widen(carry, c, head_dim)
            pre[step + 1, c] = wide * pre[step, c] + loc
            keep[step + 1, c] = wide * keep[step, c]


def in_block(back, dims, len_ref, x_ref, p_ref, q_ref, dt_ref, skip_ref, work, inside, fexp):
    nblocks, heads, groups, head_dim = dims
    cum_s, cum_t, dt_t, fout_s = work
    npair = heads * head_dim // LANES
    per = LANES // head_dim
    pair_group = npair // groups
    seg_of = seg_maker(len_ref)
    slab = lax.axis_index("seq") * (nblocks * SPAN)
    dim0 = lax.broadcasted_iota(jnp.int32, (SPAN, SPAN), 0)
    dim1 = lax.broadcasted_iota(jnp.int32, (SPAN, SPAN), 1)
    lane = lax.broadcasted_iota(jnp.int32, (1, LANES), 1)

    def one(b, _):
        start = pl.multiple_of(b * SPAN, SPAN)
        rows = pl.ds(start, SPAN)
        seg_i = seg_of(slab + start + dim0)
        seg_j = seg_of(slab + start + dim1)
        order = (dim1 >= dim0) if back else (dim1 <= dim0)
        bias = jnp.where((seg_i == seg_j) & order, 0.0, -jnp.inf)
        cum = cum_s[rows, :]
        dt = dt_ref[rows, :]
        f_out = fout_s[rows, :]
        for g in range(groups):
            gl = slice(g * LANES, (g + 1) * LANES)
            score = lax.dot_general(p_ref[rows, gl], q_ref[rows, gl], (((1,), (1,)), ((), ())),
                                    preferred_element_type=jnp.float32)
            for c in range(g * pair_group, (g + 1) * pair_group):
                cols = slice(c * LANES, (c + 1) * LANES)
                x = x_ref[rows, cols]
                mixes, parts = [], []
                for k in range(per):
                    h = c * per + k
                    col = cum[:, h:h + 1]
                    row = cum_t[b, h:h + 1, :]
                    spread = (row - col) if back else (col - row)
                    w = jnp.exp(spread + bias) * score
                    if not back:
                        w = w * dt_t[b, h:h + 1, :]
                    mixes.append(w.astype(jnp.bfloat16))
                    mine = (lane >= k * head_dim) & (lane < (k + 1) * head_dim)
                    parts.append(jnp.where(mine, x, jnp.zeros_like(x)))
                acc = jnp.dot(jnp.concatenate(mixes, 1), jnp.concatenate(parts, 0),
                              preferred_element_type=jnp.float32)
                if back:
                    acc = acc * widen(dt, c, head_dim)
                inside[c, rows, :] = acc + widen(skip_ref[...], c, head_dim) * x.astype(jnp.float32)
                fexp[c, rows, :] = widen(f_out, c, head_dim)
        return 0

    lax.fori_loop(0, nblocks, one, 0)


def back_kernel(dims, len_ref, x_ref, p_ref, q_ref, dt_ref, decay_ref, skip_ref,
                inside, fexp, pre, keep, *work):
    local_states(True, dims, len_ref, x_ref, q_ref, dt_ref, decay_ref, work, pre, keep)
    in_block(True, dims, len_ref, x_ref, p_ref, q_ref, dt_ref, skip_ref, work, inside, fexp)


HOP_CHUNKS = 5


def chain_kernel(count, dims, len_ref, x_ref, p_ref, q_ref, dt_ref, decay_ref, skip_ref,
                 pb_ref, inside_b, fexp_b, pre_b, keep_b,
                 out_ref, grad_ref, *scratch):
    work, rest = scratch[:4], scratch[4:]
    inside, fexp, pre, keep, inbox, outbox, in_b, out_b, s_sem, r_sem, sb_sem, rb_sem = rest
    nblocks, heads, groups, head_dim = dims
    npair = heads * head_dim // LANES
    pair_group = npair // groups
    me = lax.axis_index("seq")
    low, high = me == 0, me == count - 1

    barrier = pltpu.get_barrier_semaphore()

    @pl.when(jnp.logical_not(low))
    def _():
        pl.semaphore_signal(barrier, inc=1, device_id={"seq": me - 1}, device_id_type=MESH)

    @pl.when(jnp.logical_not(high))
    def _():
        pl.semaphore_signal(barrier, inc=1, device_id={"seq": me + 1}, device_id_type=MESH)

    local_states(False, dims, len_ref, x_ref, q_ref, dt_ref, decay_ref, work, pre, keep)

    @pl.when(low)
    def _():
        inbox[...] = jnp.zeros_like(inbox)

    @pl.when(high)
    def _():
        in_b[...] = jnp.zeros_like(in_b)

    pl.semaphore_wait(barrier, jnp.where(low, 0, 1) + jnp.where(high, 0, 1))

    def hop(back, c):
        return pltpu.make_async_remote_copy(
            src_ref=(out_b if back else outbox).at[c], dst_ref=(in_b if back else inbox).at[c],
            send_sem=(sb_sem if back else s_sem).at[c], recv_sem=(rb_sem if back else r_sem).at[c],
            device_id={"seq": me - 1 if back else me + 1}, device_id_type=MESH)

    def relay(back, c):
        first, last = (high, low) if back else (low, high)
        kp, pr = (keep_b, pre_b) if back else (keep, pre)

        @pl.when(jnp.logical_not(first))
        def _():
            hop(back, c).wait_recv()

        @pl.when(jnp.logical_not(last))
        def _():
            state = (in_b if back else inbox)[c].astype(jnp.float32)
            (out_b if back else outbox)[c] = (kp[nblocks, c] * state + pr[nblocks, c]).astype(jnp.bfloat16)
            hop(back, c).start()

    def finish(back, c):
        kp, pr, ins, fx, vec, out = (
            (keep_b, pre_b, inside_b, fexp_b, pb_ref, grad_ref) if back
            else (keep, pre, inside, fexp, p_ref, out_ref))
        g = c // pair_group
        cols = pl.ds(pl.multiple_of(c * LANES, LANES), LANES)
        gl = pl.ds(pl.multiple_of(g * LANES, LANES), LANES)
        state = (in_b if back else inbox)[c].astype(jnp.float32)
        for step in range(nblocks):
            b = nblocks - 1 - step if back else step
            rows = slice(b * SPAN, (b + 1) * SPAN)
            entering = (kp[step, c] * state + pr[step, c]).astype(jnp.bfloat16)
            y = jnp.dot(vec[rows, gl], entering, preferred_element_type=jnp.float32)
            out[rows, cols] = (ins[c, rows, :] + fx[c, rows, :] * y).astype(jnp.bfloat16)

    lag = (2 * me - (count - 1)) * HOP_CHUNKS
    up_first = lag < 0
    gap = jnp.where(up_first, -lag, lag)
    block_at = jnp.where(gap >= npair, npair, 0)

    def step_of(i, _):
        @pl.when(i == block_at)
        def _():
            in_block(False, dims, len_ref, x_ref, p_ref, q_ref, dt_ref, skip_ref, work, inside, fexp)

        for back in (False, True):
            leads = jnp.logical_not(up_first) if back else up_first
            c = i - jnp.where(leads, 0, gap)

            @pl.when((c >= 0) & (c < npair))
            def _(back=back, c=c):
                relay(back, c)

            done = jnp.where(leads, i - npair, c)

            @pl.when((done >= 0) & (done < npair))
            def _(back=back, done=done):
                finish(back, done)

        return 0

    lax.fori_loop(0, npair + jnp.maximum(gap, npair), step_of, 0)

    def drain(c, _):
        @pl.when(jnp.logical_not(high))
        def _():
            hop(False, c).wait_send()

        @pl.when(jnp.logical_not(low))
        def _():
            hop(True, c).wait_send()

        return 0

    lax.fori_loop(0, npair, drain, 0)


def sizes_of(x, p_vec, dt):
    tokens, width = x.shape
    heads = dt.shape[1]
    dims = (tokens // SPAN, heads, p_vec.shape[1] // LANES, width // heads)
    nblocks, npair = dims[0], width // LANES
    f32 = jnp.float32
    work = [pltpu.VMEM((tokens, heads), f32), pltpu.VMEM((nblocks, heads, SPAN), f32),
            pltpu.VMEM((nblocks, heads, SPAN), f32), pltpu.VMEM((tokens, heads), f32)]
    kept = [(npair, tokens, LANES), (npair, tokens, LANES),
            (nblocks + 1, npair, LANES, LANES), (nblocks + 1, npair, 1, LANES)]
    return dims, npair, work, kept


VM = pl.BlockSpec(memory_space=pltpu.VMEM)
SM = pl.BlockSpec(memory_space=pltpu.SMEM)


def back_parts(lengths, x, p_vec, q_vec, dt, decay, skip):
    dims, _, work, kept = sizes_of(x, p_vec, dt)
    return pl.pallas_call(
        functools.partial(back_kernel, dims),
        out_shape=[jax.ShapeDtypeStruct(k, jnp.float32) for k in kept],
        in_specs=[SM] + [VM] * 6,
        out_specs=[VM] * 4,
        scratch_shapes=work,
        compiler_params=pltpu.CompilerParams(vmem_limit_bytes=24 * 1024 * 1024),
        cost_estimate=pl.CostEstimate(flops=15_000_000_000, bytes_accessed=16_000_000, transcendentals=0),
        name="back_parts",
    )(lengths, x, p_vec, q_vec, dt, decay, skip)


def chains(lengths, x, p_vec, q_vec, dt, decay, skip, p_back, parts):
    dims, npair, work, kept = sizes_of(x, p_vec, dt)
    box = pltpu.VMEM((npair, LANES, LANES), jnp.bfloat16)
    sem = pltpu.SemaphoreType.DMA((npair,))
    return pl.pallas_call(
        functools.partial(chain_kernel, lax.axis_size("seq"), dims),
        out_shape=[jax.ShapeDtypeStruct(x.shape, jnp.bfloat16)] * 2,
        in_specs=[SM] + [VM] * 11,
        out_specs=[VM] * 2,
        scratch_shapes=work + [pltpu.VMEM(k, jnp.float32) for k in kept] + [box] * 4 + [sem] * 4,
        compiler_params=pltpu.CompilerParams(
            collective_id=0, has_side_effects=True, vmem_limit_bytes=56 * 1024 * 1024),
        cost_estimate=pl.CostEstimate(flops=40_000_000_000, bytes_accessed=40_000_000, transcendentals=0),
        name="chains",
    )(lengths, x, p_vec, q_vec, dt, decay, skip, p_back, *parts)


def body(
    hidden_next, values_next, seg_next, proj_bc, proj_dt, dt_bias, decay_rate, skip_gain,
    bc_prev, dt_prev, seg_prev, grad_prev,
):
    tokens_dev = hidden_next.shape[0]
    bc_width = proj_bc.shape[1]
    heads_all = proj_dt.shape[1]
    fsdp_count = lax.axis_size("fsdp")
    fsdp_place = lax.axis_index("fsdp")
    seq_count = lax.axis_size("seq")
    heads_dev = heads_all // fsdp_count
    state_dim = bc_width // (2 * GW)
    per_group = heads_all // GW
    groups_dev = max(1, heads_dev // per_group)
    first_head = fsdp_place * heads_dev
    first_group = first_head // per_group
    rows_dev = proj_bc.shape[0]
    half = bc_width // 2
    gw = groups_dev * state_dim

    pieces = []
    for f in range(fsdp_count):
        g0 = (f * heads_dev // per_group) * state_dim
        pieces += [proj_bc[:, g0:g0 + gw], proj_bc[:, half + g0:half + g0 + gw],
                   proj_dt[:, f * heads_dev:(f + 1) * heads_dev]]
    cols = 2 * gw + heads_dev
    weights = lax.all_gather(jnp.concatenate(pieces, axis=1), "seq", axis=0, tiled=True)

    decay = lax.dynamic_slice_in_dim(decay_rate, first_head, heads_dev, 0)[None]
    skip = lax.dynamic_slice_in_dim(skip_gain, first_head, heads_dev, 0)[None]
    bias = lax.dynamic_slice_in_dim(dt_bias, first_head, heads_dev, 0)[None]

    b_prev = lax.dynamic_slice_in_dim(bc_prev, first_group * state_dim, gw, 1)
    c_prev = lax.dynamic_slice_in_dim(bc_prev, half + first_group * state_dim, gw, 1)
    parts = back_parts(seg_prev, grad_prev, b_prev, c_prev, dt_prev, decay, skip)

    owned = lax.dynamic_slice_in_dim(
        hidden_next.reshape(tokens_dev, seq_count, fsdp_count, rows_dev), fsdp_place, 1, 2
    ).reshape(tokens_dev, seq_count * rows_dev)
    owned, parts = lax.optimization_barrier((owned, parts))
    if fsdp_count == 2:
        other = lax.dynamic_slice_in_dim(weights, (1 - fsdp_place) * cols, cols, 1)
        mine = lax.dynamic_slice_in_dim(weights, fsdp_place * cols, cols, 1)
        away = lax.ppermute(jnp.dot(owned, other, preferred_element_type=jnp.float32),
                            "fsdp", [(0, 1), (1, 0)])
        sums = jnp.dot(owned, mine, preferred_element_type=jnp.float32) + away
    else:
        sums = lax.psum_scatter(jnp.dot(owned, weights, preferred_element_type=jnp.float32),
                                "fsdp", scatter_dimension=1, tiled=True)
    b_next = sums[:, :gw].astype(jnp.bfloat16)
    c_next = sums[:, gw:2 * gw].astype(jnp.bfloat16)
    dt_next = jax.nn.softplus(sums[:, 2 * gw:] + bias)
    out_next, grad_values = chains(
        seg_next, values_next, c_next, b_next, dt_next, decay, skip, b_prev, parts)
    return (out_next, grad_values)


def solution(mesh):
    in_specs = (
        P("seq", None), P("seq", "fsdp"), P(), P(("seq", "fsdp"), None), P(("seq", "fsdp"), None),
        P(), P(), P(), P("seq", None), P("seq", "fsdp"), P(), P("seq", "fsdp"),
    )
    out_specs = (P("seq", "fsdp"), P("seq", "fsdp"))
    return jax.shard_map(body, mesh=mesh, in_specs=in_specs, out_specs=out_specs, check_vma=False)
```

```python
import functools

import jax
import jax.numpy as jnp
from jax import lax
from jax.experimental import pallas as pl
from jax.experimental.pallas import tpu as pltpu
from jax.sharding import PartitionSpec as P

GW = 4
SPAN = 128
LANES = 128
MESH = pl.DeviceIdType.MESH


def widen(a, c, head_dim):
    per = LANES // head_dim
    lane = lax.broadcasted_iota(jnp.int32, (1, LANES), 1)
    res = a[:, c * per:c * per + 1]
    for k in range(1, per):
        res = jnp.where(lane >= k * head_dim, a[:, c * per + k:c * per + k + 1], res)
    return jnp.broadcast_to(res, (a.shape[0], LANES))


def seg_maker(len_ref):
    bound = []
    total = jnp.int32(0)
    for k in range(len_ref.shape[0] - 1):
        total = total + len_ref[k]
        bound.append(total)

    def seg_of(pos):
        s = jnp.zeros_like(pos)
        for b in bound:
            s = s + (b <= pos).astype(jnp.int32)
        return s

    return seg_of


def local_states(back, dims, len_ref, x_ref, q_ref, dt_ref, decay_ref, work, pre, keep):
    nblocks, heads, groups, head_dim = dims
    cum_s, cum_t, dt_t, fout_s = work
    npair = heads * head_dim // LANES
    pair_group = npair // groups
    seg_of = seg_maker(len_ref)
    slab = lax.axis_index("seq") * (nblocks * SPAN)
    dim0 = lax.broadcasted_iota(jnp.int32, (SPAN, SPAN), 0)
    dim1 = lax.broadcasted_iota(jnp.int32, (SPAN, SPAN), 1)
    tril = (dim0 >= dim1).astype(jnp.float32)
    for c in range(npair):
        pre[0, c] = jnp.zeros((LANES, LANES), jnp.float32)
        keep[0, c] = jnp.ones((1, LANES), jnp.float32)
    for step in range(nblocks):
        b = nblocks - 1 - step if back else step
        rows = slice(b * SPAN, (b + 1) * SPAN)
        dt = dt_ref[rows, :]
        cum = jnp.dot(tril, -(dt * decay_ref[...]), precision=lax.Precision.HIGHEST,
                      preferred_element_type=jnp.float32)
        end = cum[SPAN - 1:SPAN, :]
        cum_s[rows, :] = cum
        cum_t[b] = cum.T
        dt_t[b] = dt.T
        seg = seg_of(slab + b * SPAN + lax.broadcasted_iota(jnp.int32, (SPAN, heads), 0))
        edge = slab + b * SPAN + lax.broadcasted_iota(jnp.int32, (1, heads), 0) * 0
        seg_e = seg_of(edge + (SPAN - 1))
        seg_b = jnp.where(edge == 0, 0, seg_of(edge - 1))
        send = jnp.where(seg == seg_e, jnp.exp(end - cum), 0.0) * dt
        read = jnp.where(seg == seg_b, jnp.exp(cum), 0.0)
        carry = jnp.where(seg_e == seg_b, jnp.exp(end), 0.0)
        f_in = read if back else send
        fout_s[rows, :] = send if back else read
        qt = [q_ref[rows, g * LANES:(g + 1) * LANES].T for g in range(groups)]
        for c in range(npair):
            cols = slice(c * LANES, (c + 1) * LANES)
            sent = (x_ref[rows, cols].astype(jnp.float32) * widen(f_in, c, head_dim)).astype(jnp.bfloat16)
            loc = jnp.dot(qt[c // pair_group], sent, preferred_element_type=jnp.float32)
            wide = widen(carry, c, head_dim)
            pre[step + 1, c] = wide * pre[step, c] + loc
            keep[step + 1, c] = wide * keep[step, c]


def in_block(back, dims, len_ref, x_ref, p_ref, q_ref, dt_ref, skip_ref, work, inside, fexp):
    nblocks, heads, groups, head_dim = dims
    cum_s, cum_t, dt_t, fout_s = work
    npair = heads * head_dim // LANES
    per = LANES // head_dim
    pair_group = npair // groups
    seg_of = seg_maker(len_ref)
    slab = lax.axis_index("seq") * (nblocks * SPAN)
    dim0 = lax.broadcasted_iota(jnp.int32, (SPAN, SPAN), 0)
    dim1 = lax.broadcasted_iota(jnp.int32, (SPAN, SPAN), 1)
    lane = lax.broadcasted_iota(jnp.int32, (1, LANES), 1)

    def one(b, _):
        start = pl.multiple_of(b * SPAN, SPAN)
        rows = pl.ds(start, SPAN)
        seg_i = seg_of(slab + start + dim0)
        seg_j = seg_of(slab + start + dim1)
        order = (dim1 >= dim0) if back else (dim1 <= dim0)
        bias = jnp.where((seg_i == seg_j) & order, 0.0, -jnp.inf)
        cum = cum_s[rows, :]
        dt = dt_ref[rows, :]
        f_out = fout_s[rows, :]
        for g in range(groups):
            gl = slice(g * LANES, (g + 1) * LANES)
            score = lax.dot_general(p_ref[rows, gl], q_ref[rows, gl], (((1,), (1,)), ((), ())),
                                    preferred_element_type=jnp.float32)
            for c in range(g * pair_group, (g + 1) * pair_group):
                cols = slice(c * LANES, (c + 1) * LANES)
                x = x_ref[rows, cols]
                mixes, parts = [], []
                for k in range(per):
                    h = c * per + k
                    col = cum[:, h:h + 1]
                    row = cum_t[b, h:h + 1, :]
                    spread = (row - col) if back else (col - row)
                    w = jnp.exp(spread + bias) * score
                    if not back:
                        w = w * dt_t[b, h:h + 1, :]
                    mixes.append(w.astype(jnp.bfloat16))
                    mine = (lane >= k * head_dim) & (lane < (k + 1) * head_dim)
                    parts.append(jnp.where(mine, x, jnp.zeros_like(x)))
                acc = jnp.dot(jnp.concatenate(mixes, 1), jnp.concatenate(parts, 0),
                              preferred_element_type=jnp.float32)
                if back:
                    acc = acc * widen(dt, c, head_dim)
                inside[c, rows, :] = acc + widen(skip_ref[...], c, head_dim) * x.astype(jnp.float32)
                fexp[c, rows, :] = widen(f_out, c, head_dim)
        return 0

    lax.fori_loop(0, nblocks, one, 0)


def back_kernel(dims, len_ref, x_ref, p_ref, q_ref, dt_ref, decay_ref, skip_ref,
                inside, fexp, pre, keep, *work):
    local_states(True, dims, len_ref, x_ref, q_ref, dt_ref, decay_ref, work, pre, keep)
    in_block(True, dims, len_ref, x_ref, p_ref, q_ref, dt_ref, skip_ref, work, inside, fexp)


HOP_CHUNKS = 5


def chain_kernel(count, dims, len_ref, x_ref, p_ref, q_ref, dt_ref, decay_ref, skip_ref,
                 pb_ref, inside_b, fexp_b, pre_b, keep_b,
                 out_ref, grad_ref, *scratch):
    work, rest = scratch[:4], scratch[4:]
    inside, fexp, pre, keep, inbox, outbox, in_b, out_b, s_sem, r_sem, sb_sem, rb_sem = rest
    nblocks, heads, groups, head_dim = dims
    npair = heads * head_dim // LANES
    pair_group = npair // groups
    me = lax.axis_index("seq")
    low, high = me == 0, me == count - 1

    barrier = pltpu.get_barrier_semaphore()

    @pl.when(jnp.logical_not(low))
    def _():
        pl.semaphore_signal(barrier, inc=1, device_id={"seq": me - 1}, device_id_type=MESH)

    @pl.when(jnp.logical_not(high))
    def _():
        pl.semaphore_signal(barrier, inc=1, device_id={"seq": me + 1}, device_id_type=MESH)

    local_states(False, dims, len_ref, x_ref, q_ref, dt_ref, decay_ref, work, pre, keep)

    @pl.when(low)
    def _():
        inbox[...] = jnp.zeros_like(inbox)

    @pl.when(high)
    def _():
        in_b[...] = jnp.zeros_like(in_b)

    pl.semaphore_wait(barrier, jnp.where(low, 0, 1) + jnp.where(high, 0, 1))

    def hop(back, c):
        return pltpu.make_async_remote_copy(
            src_ref=(out_b if back else outbox).at[c], dst_ref=(in_b if back else inbox).at[c],
            send_sem=(sb_sem if back else s_sem).at[c], recv_sem=(rb_sem if back else r_sem).at[c],
            device_id={"seq": me - 1 if back else me + 1}, device_id_type=MESH)

    def relay(back, c):
        first, last = (high, low) if back else (low, high)
        kp, pr = (keep_b, pre_b) if back else (keep, pre)

        @pl.when(jnp.logical_not(first))
        def _():
            hop(back, c).wait_recv()

        @pl.when(jnp.logical_not(last))
        def _():
            state = (in_b if back else inbox)[c].astype(jnp.float32)
            (out_b if back else outbox)[c] = (kp[nblocks, c] * state + pr[nblocks, c]).astype(jnp.bfloat16)
            hop(back, c).start()

    def finish(back, c):
        kp, pr, ins, fx, vec, out = (
            (keep_b, pre_b, inside_b, fexp_b, pb_ref, grad_ref) if back
            else (keep, pre, inside, fexp, p_ref, out_ref))
        g = c // pair_group
        cols = pl.ds(pl.multiple_of(c * LANES, LANES), LANES)
        gl = pl.ds(pl.multiple_of(g * LANES, LANES), LANES)
        state = (in_b if back else inbox)[c].astype(jnp.float32)
        for step in range(nblocks):
            b = nblocks - 1 - step if back else step
            rows = slice(b * SPAN, (b + 1) * SPAN)
            entering = (kp[step, c] * state + pr[step, c]).astype(jnp.bfloat16)
            y = jnp.dot(vec[rows, gl], entering, preferred_element_type=jnp.float32)
            out[rows, cols] = (ins[c, rows, :] + fx[c, rows, :] * y).astype(jnp.bfloat16)

    lag = (2 * me - (count - 1)) * HOP_CHUNKS
    up_first = lag < 0
    gap = jnp.where(up_first, -lag, lag)
    block_at = jnp.where(gap >= npair, npair, 0)

    def step_of(i, _):
        @pl.when(i == block_at)
        def _():
            in_block(False, dims, len_ref, x_ref, p_ref, q_ref, dt_ref, skip_ref, work, inside, fexp)

        for back in (False, True):
            leads = jnp.logical_not(up_first) if back else up_first
            c = i - jnp.where(leads, 0, gap)

            @pl.when((c >= 0) & (c < npair))
            def _(back=back, c=c):
                relay(back, c)

            done = jnp.where(leads, i - npair, c)

            @pl.when((done >= 0) & (done < npair))
            def _(back=back, done=done):
                finish(back, done)

        return 0

    lax.fori_loop(0, npair + jnp.maximum(gap, npair), step_of, 0)

    def drain(c, _):
        @pl.when(jnp.logical_not(high))
        def _():
            hop(False, c).wait_send()

        @pl.when(jnp.logical_not(low))
        def _():
            hop(True, c).wait_send()

        return 0

    lax.fori_loop(0, npair, drain, 0)


def sizes_of(x, p_vec, dt):
    tokens, width = x.shape
    heads = dt.shape[1]
    dims = (tokens // SPAN, heads, p_vec.shape[1] // LANES, width // heads)
    nblocks, npair = dims[0], width // LANES
    f32 = jnp.float32
    work = [pltpu.VMEM((tokens, heads), f32), pltpu.VMEM((nblocks, heads, SPAN), f32),
            pltpu.VMEM((nblocks, heads, SPAN), f32), pltpu.VMEM((tokens, heads), f32)]
    kept = [(npair, tokens, LANES), (npair, tokens, LANES),
            (nblocks + 1, npair, LANES, LANES), (nblocks + 1, npair, 1, LANES)]
    return dims, npair, work, kept


VM = pl.BlockSpec(memory_space=pltpu.VMEM)
SM = pl.BlockSpec(memory_space=pltpu.SMEM)


def back_parts(lengths, x, p_vec, q_vec, dt, decay, skip):
    dims, _, work, kept = sizes_of(x, p_vec, dt)
    return pl.pallas_call(
        functools.partial(back_kernel, dims),
        out_shape=[jax.ShapeDtypeStruct(k, jnp.float32) for k in kept],
        in_specs=[SM] + [VM] * 6,
        out_specs=[VM] * 4,
        scratch_shapes=work,
        compiler_params=pltpu.CompilerParams(vmem_limit_bytes=24 * 1024 * 1024),
        cost_estimate=pl.CostEstimate(flops=15_000_000_000, bytes_accessed=16_000_000, transcendentals=0),
        name="back_parts",
    )(lengths, x, p_vec, q_vec, dt, decay, skip)


def chains(lengths, x, p_vec, q_vec, dt, decay, skip, p_back, parts):
    dims, npair, work, kept = sizes_of(x, p_vec, dt)
    box = pltpu.VMEM((npair, LANES, LANES), jnp.bfloat16)
    sem = pltpu.SemaphoreType.DMA((npair,))
    return pl.pallas_call(
        functools.partial(chain_kernel, lax.axis_size("seq"), dims),
        out_shape=[jax.ShapeDtypeStruct(x.shape, jnp.bfloat16)] * 2,
        in_specs=[SM] + [VM] * 11,
        out_specs=[VM] * 2,
        scratch_shapes=work + [pltpu.VMEM(k, jnp.float32) for k in kept] + [box] * 4 + [sem] * 4,
        compiler_params=pltpu.CompilerParams(
            collective_id=0, has_side_effects=True, vmem_limit_bytes=56 * 1024 * 1024),
        cost_estimate=pl.CostEstimate(flops=40_000_000_000, bytes_accessed=40_000_000, transcendentals=0),
        name="chains",
    )(lengths, x, p_vec, q_vec, dt, decay, skip, p_back, *parts)


PIECES = 4


def gather_kernel(count, h_ref, w_ref, bc_ref, dt_ref,
                  held, acc, bc_out, bc_in, dt_out, dt_in,
                  ring_s, ring_r, side_s, side_r, x_s, x_r):
    me, f = lax.axis_index("seq"), lax.axis_index("fsdp")
    n = count // 2
    half_ring = n // 2
    core, chip = me % 2, me // 2
    r = jnp.where(chip % 2 == 0, chip // 2, n - 1 - chip // 2)
    rows = w_ref.shape[0]
    piece = rows // PIECES
    wide = bc_ref.shape[1]

    def id_of(pos, which):
        p = (pos + 2 * n) % n
        up = p < half_ring
        return jnp.where(up, p * 2, (n - 1 - p) * 2 + 1) * 2 + which

    nxt, prv, partner = id_of(r + 1, core), id_of(r - 1, core), chip * 2 + 1 - core

    barrier = pltpu.get_barrier_semaphore()
    for peer in (nxt, prv, partner):
        pl.semaphore_signal(barrier, inc=1, device_id={"seq": peer}, device_id_type=MESH)
    pl.semaphore_signal(barrier, inc=1, device_id={"fsdp": 1 - f}, device_id_type=MESH)
    pl.semaphore_wait(barrier, 4)

    def part(p):
        return pl.ds(p * piece, piece)

    def origin(step, p, which):
        return id_of(r - step if p < PIECES // 2 else r + step, which)

    def ring_copy(step, p, src):
        return pltpu.make_async_remote_copy(
            src_ref=src, dst_ref=held.at[origin(step, p, core), part(p), :],
            send_sem=ring_s.at[step, p], recv_sem=ring_r.at[step, p],
            device_id={"seq": nxt if p < PIECES // 2 else prv}, device_id_type=MESH)

    def side_copy(step, p, src):
        return pltpu.make_async_remote_copy(
            src_ref=src, dst_ref=held.at[origin(step, p, core), part(p), :],
            send_sem=side_s.at[step, p], recv_sem=side_r.at[step, p],
            device_id={"seq": partner}, device_id_type=MESH)

    def landed(step, p):
        return held.at[origin(step, p, core), part(p), :]

    for p in range(PIECES):
        ring_copy(0, p, w_ref.at[part(p), :]).start()
    for p in range(PIECES):
        side_copy(0, p, w_ref.at[part(p), :]).start()

    def columns(seq_index, first):
        start = (seq_index * 2 + f) * rows + first
        return h_ref[:, pl.ds(pl.multiple_of(start, rows // 2), rows // 2)]

    def mac(step, which):
        half = rows // 2
        lo, hi = origin(step, 0, which), origin(step, PIECES - 1, which)
        left = jnp.concatenate([columns(lo, 0), columns(hi, half)], axis=1)
        right = jnp.concatenate([held[lo, 0:half, :], held[hi, half:, :]], axis=0)
        acc[...] += jnp.dot(left, right, preferred_element_type=jnp.float32)

    acc[...] = jnp.dot(jnp.concatenate([columns(me, 0), columns(me, rows // 2)], axis=1), w_ref[...],
                       preferred_element_type=jnp.float32)

    def one(step, _):
        for p in (0, PIECES // 2, 1, PIECES // 2 + 1):
            ring_copy(step, p, landed(step, p)).wait_recv()

            @pl.when(step < n - 2)
            def _(p=p):
                ring_copy(step + 1, p, landed(step + 1, p)).start()

            side_copy(step + 1, p, landed(step + 1, p)).start()
        mac(step + 1, core)
        for p in range(PIECES):
            side_copy(step, p, landed(step, p)).wait_recv()
        mac(step, 1 - core)
        return 0

    lax.fori_loop(0, n - 1, one, 0)
    for p in range(PIECES):
        side_copy(n - 1, p, landed(n - 1, p)).wait_recv()
    mac(n - 1, 1 - core)

    def cross(src, dst, k):
        return pltpu.make_async_remote_copy(
            src_ref=src, dst_ref=dst, send_sem=x_s.at[k], recv_sem=x_r.at[k],
            device_id={"fsdp": 1 - f}, device_id_type=MESH)

    def side_of(which):
        return pl.ds(pl.multiple_of(which * wide, wide), wide)

    bc_out[...] = acc[:, side_of(1 - f)].astype(jnp.bfloat16)
    dt_out[...] = acc[:, 2 * wide:]
    cross(bc_out, bc_in, 0).start()
    cross(dt_out, dt_in, 1).start()

    def drain(step, _):
        for p in range(PIECES):
            @pl.when(step < n - 1)
            def _(p=p):
                ring_copy(step, p, landed(step, p)).wait_send()

            side_copy(step, p, landed(step, p)).wait_send()
        return 0

    lax.fori_loop(0, n, drain, 0)
    cross(bc_out, bc_in, 0).wait()
    bc_ref[...] = (acc[:, side_of(f)] + bc_in[...].astype(jnp.float32)).astype(jnp.bfloat16)
    cross(dt_out, dt_in, 1).wait()
    dt_ref[...] = acc[:, 2 * wide:] + dt_in[...]


def gathered_sums(hidden, shard, wide):
    count = lax.axis_size("seq")
    tokens, total = hidden.shape[0], shard.shape[1]
    f32, bf16 = jnp.float32, jnp.bfloat16
    n = count // 2
    dma = pltpu.SemaphoreType.DMA
    return pl.pallas_call(
        functools.partial(gather_kernel, count),
        out_shape=[jax.ShapeDtypeStruct((tokens, wide), bf16),
                   jax.ShapeDtypeStruct((tokens, total - 2 * wide), f32)],
        in_specs=[VM] * 2,
        out_specs=[VM] * 2,
        scratch_shapes=[
            pltpu.VMEM((count,) + shard.shape, bf16),
            pltpu.VMEM((tokens, total), f32),
            pltpu.VMEM((tokens, wide), bf16), pltpu.VMEM((tokens, wide), bf16),
            pltpu.VMEM((tokens, total - 2 * wide), f32), pltpu.VMEM((tokens, total - 2 * wide), f32),
            dma((n, PIECES)), dma((n, PIECES)), dma((n, PIECES)), dma((n, PIECES)), dma((2,)), dma((2,)),
        ],
        compiler_params=pltpu.CompilerParams(
            collective_id=1, has_side_effects=True, vmem_limit_bytes=32 * 1024 * 1024),
        cost_estimate=pl.CostEstimate(flops=40_000_000_000, bytes_accessed=40_000_000, transcendentals=0),
        name="gather_project",
    )(hidden, shard)


def body(
    hidden_next, values_next, seg_next, proj_bc, proj_dt, dt_bias, decay_rate, skip_gain,
    bc_prev, dt_prev, seg_prev, grad_prev,
):
    tokens_dev = hidden_next.shape[0]
    bc_width = proj_bc.shape[1]
    heads_all = proj_dt.shape[1]
    fsdp_count = lax.axis_size("fsdp")
    fsdp_place = lax.axis_index("fsdp")
    seq_count = lax.axis_size("seq")
    heads_dev = heads_all // fsdp_count
    state_dim = bc_width // (2 * GW)
    per_group = heads_all // GW
    groups_dev = max(1, heads_dev // per_group)
    first_head = fsdp_place * heads_dev
    first_group = first_head // per_group
    rows_dev = proj_bc.shape[0]
    half = bc_width // 2
    gw = groups_dev * state_dim

    blocks = []
    for f in range(fsdp_count):
        g0 = (f * heads_dev // per_group) * state_dim
        blocks.append([proj_bc[:, g0:g0 + gw], proj_bc[:, half + g0:half + g0 + gw]])
    ring = fsdp_count == 2 and seq_count % 4 == 0 and rows_dev % (2 * LANES) == 0 and heads_all == LANES
    if ring:
        shard = jnp.concatenate([*blocks[0], *blocks[1], proj_dt], axis=1)
        bc_next, dt_sum = gathered_sums(hidden_next, shard, 2 * gw)
        dt_sum = lax.dynamic_slice_in_dim(dt_sum, first_head, heads_dev, 1)
    else:
        pieces = []
        for f in range(fsdp_count):
            pieces += [*blocks[f], proj_dt[:, f * heads_dev:(f + 1) * heads_dev]]
        weights = lax.all_gather(jnp.concatenate(pieces, axis=1), "seq", axis=0, tiled=True)
        owned = lax.dynamic_slice_in_dim(
            hidden_next.reshape(tokens_dev, seq_count, fsdp_count, rows_dev), fsdp_place, 1, 2
        ).reshape(tokens_dev, seq_count * rows_dev)
        sums = lax.psum_scatter(jnp.dot(owned, weights, preferred_element_type=jnp.float32),
                                "fsdp", scatter_dimension=1, tiled=True)
        bc_next, dt_sum = sums[:, :2 * gw].astype(jnp.bfloat16), sums[:, 2 * gw:]

    decay = lax.dynamic_slice_in_dim(decay_rate, first_head, heads_dev, 0)[None]
    skip = lax.dynamic_slice_in_dim(skip_gain, first_head, heads_dev, 0)[None]
    bias = lax.dynamic_slice_in_dim(dt_bias, first_head, heads_dev, 0)[None]

    bc_prev, bc_next = lax.optimization_barrier((bc_prev, bc_next))
    b_prev = lax.dynamic_slice_in_dim(bc_prev, first_group * state_dim, gw, 1)
    c_prev = lax.dynamic_slice_in_dim(bc_prev, half + first_group * state_dim, gw, 1)
    parts = back_parts(seg_prev, grad_prev, b_prev, c_prev, dt_prev, decay, skip)
    b_next, c_next = bc_next[:, :gw], bc_next[:, gw:]
    dt_next = jax.nn.softplus(dt_sum + bias)
    out_next, grad_values = chains(
        seg_next, values_next, c_next, b_next, dt_next, decay, skip, b_prev, parts)
    return (out_next, grad_values)


def solution(mesh):
    in_specs = (
        P("seq", None), P("seq", "fsdp"), P(), P(("seq", "fsdp"), None), P(("seq", "fsdp"), None),
        P(), P(), P(), P("seq", None), P("seq", "fsdp"), P(), P("seq", "fsdp"),
    )
    out_specs = (P("seq", "fsdp"), P("seq", "fsdp"))
    return jax.shard_map(body, mesh=mesh, in_specs=in_specs, out_specs=out_specs, check_vma=False)
```

```python
import functools

import jax
import jax.numpy as jnp
from jax import lax
from jax.experimental import pallas as pl
from jax.experimental.pallas import tpu as pltpu
from jax.sharding import PartitionSpec as P

GW = 4
SPAN = 128
LANES = 128
MESH = pl.DeviceIdType.MESH


def widen(a, c, head_dim):
    per = LANES // head_dim
    lane = lax.broadcasted_iota(jnp.int32, (1, LANES), 1)
    res = a[:, c * per:c * per + 1]
    for k in range(1, per):
        res = jnp.where(lane >= k * head_dim, a[:, c * per + k:c * per + k + 1], res)
    return jnp.broadcast_to(res, (a.shape[0], LANES))


def seg_maker(len_ref):
    bound = []
    total = jnp.int32(0)
    for k in range(len_ref.shape[0] - 1):
        total = total + len_ref[k]
        bound.append(total)

    def seg_of(pos):
        s = jnp.zeros_like(pos)
        for b in bound:
            s = s + (b <= pos).astype(jnp.int32)
        return s

    return seg_of


def local_states(back, dims, len_ref, x_ref, q_ref, dt_ref, decay_ref, work, pre, keep):
    nblocks, heads, groups, head_dim = dims
    cum_s, cum_t, dt_t, fout_s = work
    npair = heads * head_dim // LANES
    pair_group = npair // groups
    seg_of = seg_maker(len_ref)
    slab = lax.axis_index("seq") * (nblocks * SPAN)
    dim0 = lax.broadcasted_iota(jnp.int32, (SPAN, SPAN), 0)
    dim1 = lax.broadcasted_iota(jnp.int32, (SPAN, SPAN), 1)
    tril = (dim0 >= dim1).astype(jnp.float32)
    for c in range(npair):
        pre[0, c] = jnp.zeros((LANES, LANES), jnp.float32)
        keep[0, c] = jnp.ones((1, LANES), jnp.float32)
    for step in range(nblocks):
        b = nblocks - 1 - step if back else step
        rows = slice(b * SPAN, (b + 1) * SPAN)
        dt = dt_ref[rows, :]
        cum = jnp.dot(tril, -(dt * decay_ref[...]), precision=lax.Precision.HIGHEST,
                      preferred_element_type=jnp.float32)
        end = cum[SPAN - 1:SPAN, :]
        cum_s[rows, :] = cum
        cum_t[b] = cum.T
        dt_t[b] = dt.T
        seg = seg_of(slab + b * SPAN + lax.broadcasted_iota(jnp.int32, (SPAN, heads), 0))
        edge = slab + b * SPAN + lax.broadcasted_iota(jnp.int32, (1, heads), 0) * 0
        seg_e = seg_of(edge + (SPAN - 1))
        seg_b = jnp.where(edge == 0, 0, seg_of(edge - 1))
        send = jnp.where(seg == seg_e, jnp.exp(end - cum), 0.0) * dt
        read = jnp.where(seg == seg_b, jnp.exp(cum), 0.0)
        carry = jnp.where(seg_e == seg_b, jnp.exp(end), 0.0)
        f_in = read if back else send
        fout_s[rows, :] = send if back else read
        qt = [q_ref[rows, g * LANES:(g + 1) * LANES].T for g in range(groups)]
        for c in range(npair):
            cols = slice(c * LANES, (c + 1) * LANES)
            sent = (x_ref[rows, cols].astype(jnp.float32) * widen(f_in, c, head_dim)).astype(jnp.bfloat16)
            loc = jnp.dot(qt[c // pair_group], sent, preferred_element_type=jnp.float32)
            wide = widen(carry, c, head_dim)
            pre[step + 1, c] = wide * pre[step, c] + loc
            keep[step + 1, c] = wide * keep[step, c]


def in_block(back, dims, len_ref, x_ref, p_ref, q_ref, dt_ref, skip_ref, work, inside, fexp):
    nblocks, heads, groups, head_dim = dims
    cum_s, cum_t, dt_t, fout_s = work
    npair = heads * head_dim // LANES
    per = LANES // head_dim
    pair_group = npair // groups
    seg_of = seg_maker(len_ref)
    slab = lax.axis_index("seq") * (nblocks * SPAN)
    dim0 = lax.broadcasted_iota(jnp.int32, (SPAN, SPAN), 0)
    dim1 = lax.broadcasted_iota(jnp.int32, (SPAN, SPAN), 1)
    lane = lax.broadcasted_iota(jnp.int32, (1, LANES), 1)

    def one(b, _):
        start = pl.multiple_of(b * SPAN, SPAN)
        rows = pl.ds(start, SPAN)
        seg_i = seg_of(slab + start + dim0)
        seg_j = seg_of(slab + start + dim1)
        order = (dim1 >= dim0) if back else (dim1 <= dim0)
        bias = jnp.where((seg_i == seg_j) & order, 0.0, -jnp.inf)
        cum = cum_s[rows, :]
        dt = dt_ref[rows, :]
        f_out = fout_s[rows, :]
        for g in range(groups):
            gl = slice(g * LANES, (g + 1) * LANES)
            score = lax.dot_general(p_ref[rows, gl], q_ref[rows, gl], (((1,), (1,)), ((), ())),
                                    preferred_element_type=jnp.float32)
            for c in range(g * pair_group, (g + 1) * pair_group):
                cols = slice(c * LANES, (c + 1) * LANES)
                x = x_ref[rows, cols]
                mixes, parts = [], []
                for k in range(per):
                    h = c * per + k
                    col = cum[:, h:h + 1]
                    row = cum_t[b, h:h + 1, :]
                    spread = (row - col) if back else (col - row)
                    w = jnp.exp(spread + bias) * score
                    if not back:
                        w = w * dt_t[b, h:h + 1, :]
                    mixes.append(w.astype(jnp.bfloat16))
                    mine = (lane >= k * head_dim) & (lane < (k + 1) * head_dim)
                    parts.append(jnp.where(mine, x, jnp.zeros_like(x)))
                acc = jnp.dot(jnp.concatenate(mixes, 1), jnp.concatenate(parts, 0),
                              preferred_element_type=jnp.float32)
                if back:
                    acc = acc * widen(dt, c, head_dim)
                inside[c, rows, :] = acc + widen(skip_ref[...], c, head_dim) * x.astype(jnp.float32)
                fexp[c, rows, :] = widen(f_out, c, head_dim)
        return 0

    lax.fori_loop(0, nblocks, one, 0)


HOP_CHUNKS = 5


def chain_kernel(count, dims, len_ref, x_ref, p_ref, q_ref, dt_ref, decay_ref, skip_ref,
                 lenb_ref, xb_ref, pb_ref, qb_ref, dtb_ref,
                 out_ref, grad_ref, *scratch):
    work, work_b, rest = scratch[:4], scratch[4:8], scratch[12:]
    inside_b, fexp_b, pre_b, keep_b = scratch[8:12]
    inside, fexp, pre, keep, inbox, outbox, in_b, out_b, s_sem, r_sem, sb_sem, rb_sem = rest
    nblocks, heads, groups, head_dim = dims
    npair = heads * head_dim // LANES
    pair_group = npair // groups
    me = lax.axis_index("seq")
    low, high = me == 0, me == count - 1

    barrier = pltpu.get_barrier_semaphore()

    @pl.when(jnp.logical_not(low))
    def _():
        pl.semaphore_signal(barrier, inc=1, device_id={"seq": me - 1}, device_id_type=MESH)

    @pl.when(jnp.logical_not(high))
    def _():
        pl.semaphore_signal(barrier, inc=1, device_id={"seq": me + 1}, device_id_type=MESH)

    local_states(False, dims, len_ref, x_ref, q_ref, dt_ref, decay_ref, work, pre, keep)
    local_states(True, dims, lenb_ref, xb_ref, qb_ref, dtb_ref, decay_ref, work_b, pre_b, keep_b)

    @pl.when(low)
    def _():
        inbox[...] = jnp.zeros_like(inbox)

    @pl.when(high)
    def _():
        in_b[...] = jnp.zeros_like(in_b)

    pl.semaphore_wait(barrier, jnp.where(low, 0, 1) + jnp.where(high, 0, 1))

    def hop(back, c):
        return pltpu.make_async_remote_copy(
            src_ref=(out_b if back else outbox).at[c], dst_ref=(in_b if back else inbox).at[c],
            send_sem=(sb_sem if back else s_sem).at[c], recv_sem=(rb_sem if back else r_sem).at[c],
            device_id={"seq": me - 1 if back else me + 1}, device_id_type=MESH)

    def relay(back, c):
        first, last = (high, low) if back else (low, high)
        kp, pr = (keep_b, pre_b) if back else (keep, pre)

        @pl.when(jnp.logical_not(first))
        def _():
            hop(back, c).wait_recv()

        @pl.when(jnp.logical_not(last))
        def _():
            state = (in_b if back else inbox)[c].astype(jnp.float32)
            (out_b if back else outbox)[c] = (kp[nblocks, c] * state + pr[nblocks, c]).astype(jnp.bfloat16)
            hop(back, c).start()

    def finish(back, c):
        kp, pr, ins, fx, vec, out = (
            (keep_b, pre_b, inside_b, fexp_b, pb_ref, grad_ref) if back
            else (keep, pre, inside, fexp, p_ref, out_ref))
        g = c // pair_group
        cols = pl.ds(pl.multiple_of(c * LANES, LANES), LANES)
        gl = pl.ds(pl.multiple_of(g * LANES, LANES), LANES)
        state = (in_b if back else inbox)[c].astype(jnp.float32)
        for step in range(nblocks):
            b = nblocks - 1 - step if back else step
            rows = slice(b * SPAN, (b + 1) * SPAN)
            entering = (kp[step, c] * state + pr[step, c]).astype(jnp.bfloat16)
            y = jnp.dot(vec[rows, gl], entering, preferred_element_type=jnp.float32)
            out[rows, cols] = (ins[c, rows, :] + fx[c, rows, :] * y).astype(jnp.bfloat16)

    lag = (2 * me - (count - 1)) * HOP_CHUNKS
    up_first = lag < 0
    gap = jnp.where(up_first, -lag, lag)
    block_at = jnp.where(gap >= npair, npair, 0)

    def step_of(i, _):
        @pl.when(i == block_at)
        def _():
            in_block(False, dims, len_ref, x_ref, p_ref, q_ref, dt_ref, skip_ref, work, inside, fexp)
            in_block(True, dims, lenb_ref, xb_ref, pb_ref, qb_ref, dtb_ref, skip_ref, work_b, inside_b, fexp_b)

        for back in (False, True):
            leads = jnp.logical_not(up_first) if back else up_first
            c = i - jnp.where(leads, 0, gap)

            @pl.when((c >= 0) & (c < npair))
            def _(back=back, c=c):
                relay(back, c)

            done = jnp.where(leads, i - npair, c)

            @pl.when((done >= 0) & (done < npair))
            def _(back=back, done=done):
                finish(back, done)

        return 0

    lax.fori_loop(0, npair + jnp.maximum(gap, npair), step_of, 0)

    def drain(c, _):
        @pl.when(jnp.logical_not(high))
        def _():
            hop(False, c).wait_send()

        @pl.when(jnp.logical_not(low))
        def _():
            hop(True, c).wait_send()

        return 0

    lax.fori_loop(0, npair, drain, 0)


def sizes_of(x, p_vec, dt):
    tokens, width = x.shape
    heads = dt.shape[1]
    dims = (tokens // SPAN, heads, p_vec.shape[1] // LANES, width // heads)
    nblocks, npair = dims[0], width // LANES
    f32 = jnp.float32
    work = [pltpu.VMEM((tokens, heads), f32), pltpu.VMEM((nblocks, heads, SPAN), f32),
            pltpu.VMEM((nblocks, heads, SPAN), f32), pltpu.VMEM((tokens, heads), f32)]
    kept = [(npair, tokens, LANES), (npair, tokens, LANES),
            (nblocks + 1, npair, LANES, LANES), (nblocks + 1, npair, 1, LANES)]
    return dims, npair, work, kept


VM = pl.BlockSpec(memory_space=pltpu.VMEM)
SM = pl.BlockSpec(memory_space=pltpu.SMEM)


def chains(lengths, x, p_vec, q_vec, dt, decay, skip, *back):
    dims, npair, work, kept = sizes_of(x, p_vec, dt)
    box = pltpu.VMEM((npair, LANES, LANES), jnp.bfloat16)
    sem = pltpu.SemaphoreType.DMA((npair,))
    return pl.pallas_call(
        functools.partial(chain_kernel, lax.axis_size("seq"), dims),
        out_shape=[jax.ShapeDtypeStruct(x.shape, jnp.bfloat16)] * 2,
        in_specs=[SM] + [VM] * 6 + [SM] + [VM] * 4,
        out_specs=[VM] * 2,
        scratch_shapes=(work * 2 + [pltpu.VMEM(k, jnp.float32) for k in kept] * 2
                        + [box] * 4 + [sem] * 4),
        compiler_params=pltpu.CompilerParams(
            collective_id=0, has_side_effects=True, vmem_limit_bytes=56 * 1024 * 1024),
        cost_estimate=pl.CostEstimate(flops=40_000_000_000, bytes_accessed=40_000_000, transcendentals=0),
        name="chains",
    )(lengths, x, p_vec, q_vec, dt, decay, skip, *back)


PIECES = 4


def gather_kernel(count, h_ref, w_ref, bc_ref, dt_ref,
                  held, acc, bc_out, bc_in, dt_out, dt_in,
                  ring_s, ring_r, side_s, side_r, x_s, x_r):
    me, f = lax.axis_index("seq"), lax.axis_index("fsdp")
    n = count // 2
    half_ring = n // 2
    core, chip = me % 2, me // 2
    r = jnp.where(chip % 2 == 0, chip // 2, n - 1 - chip // 2)
    rows = w_ref.shape[0]
    piece = rows // PIECES
    wide = bc_ref.shape[1]

    def id_of(pos, which):
        p = (pos + 2 * n) % n
        up = p < half_ring
        return jnp.where(up, p * 2, (n - 1 - p) * 2 + 1) * 2 + which

    nxt, prv, partner = id_of(r + 1, core), id_of(r - 1, core), chip * 2 + 1 - core

    barrier = pltpu.get_barrier_semaphore()
    for peer in (nxt, prv, partner):
        pl.semaphore_signal(barrier, inc=1, device_id={"seq": peer}, device_id_type=MESH)
    pl.semaphore_signal(barrier, inc=1, device_id={"fsdp": 1 - f}, device_id_type=MESH)
    pl.semaphore_wait(barrier, 4)

    def part(p):
        return pl.ds(p * piece, piece)

    def origin(step, p, which):
        return id_of(r - step if p < PIECES // 2 else r + step, which)

    def ring_copy(step, p, src):
        return pltpu.make_async_remote_copy(
            src_ref=src, dst_ref=held.at[origin(step, p, core), part(p), :],
            send_sem=ring_s.at[step, p], recv_sem=ring_r.at[step, p],
            device_id={"seq": nxt if p < PIECES // 2 else prv}, device_id_type=MESH)

    def side_copy(step, p, src):
        return pltpu.make_async_remote_copy(
            src_ref=src, dst_ref=held.at[origin(step, p, core), part(p), :],
            send_sem=side_s.at[step, p], recv_sem=side_r.at[step, p],
            device_id={"seq": partner}, device_id_type=MESH)

    def landed(step, p):
        return held.at[origin(step, p, core), part(p), :]

    for p in range(PIECES):
        ring_copy(0, p, w_ref.at[part(p), :]).start()
    for p in range(PIECES):
        side_copy(0, p, w_ref.at[part(p), :]).start()

    def columns(seq_index, first):
        start = (seq_index * 2 + f) * rows + first
        return h_ref[:, pl.ds(pl.multiple_of(start, rows // 2), rows // 2)]

    def mac(step, which):
        half = rows // 2
        lo, hi = origin(step, 0, which), origin(step, PIECES - 1, which)
        left = jnp.concatenate([columns(lo, 0), columns(hi, half)], axis=1)
        right = jnp.concatenate([held[lo, 0:half, :], held[hi, half:, :]], axis=0)
        acc[...] += jnp.dot(left, right, preferred_element_type=jnp.float32)

    acc[...] = jnp.dot(jnp.concatenate([columns(me, 0), columns(me, rows // 2)], axis=1), w_ref[...],
                       preferred_element_type=jnp.float32)

    def one(step, _):
        for p in (0, PIECES // 2, 1, PIECES // 2 + 1):
            ring_copy(step, p, landed(step, p)).wait_recv()

            @pl.when(step < n - 2)
            def _(p=p):
                ring_copy(step + 1, p, landed(step + 1, p)).start()

            side_copy(step + 1, p, landed(step + 1, p)).start()
        mac(step + 1, core)
        for p in range(PIECES):
            side_copy(step, p, landed(step, p)).wait_recv()
        mac(step, 1 - core)
        return 0

    lax.fori_loop(0, n - 1, one, 0)
    for p in range(PIECES):
        side_copy(n - 1, p, landed(n - 1, p)).wait_recv()
    mac(n - 1, 1 - core)

    def cross(src, dst, k):
        return pltpu.make_async_remote_copy(
            src_ref=src, dst_ref=dst, send_sem=x_s.at[k], recv_sem=x_r.at[k],
            device_id={"fsdp": 1 - f}, device_id_type=MESH)

    def side_of(which):
        return pl.ds(pl.multiple_of(which * wide, wide), wide)

    bc_out[...] = acc[:, side_of(1 - f)]
    dt_out[...] = acc[:, 2 * wide:]
    cross(bc_out, bc_in, 0).start()
    cross(dt_out, dt_in, 1).start()

    def drain(step, _):
        for p in range(PIECES):
            @pl.when(step < n - 1)
            def _(p=p):
                ring_copy(step, p, landed(step, p)).wait_send()

            side_copy(step, p, landed(step, p)).wait_send()
        return 0

    lax.fori_loop(0, n, drain, 0)
    cross(bc_out, bc_in, 0).wait()
    bc_ref[...] = (acc[:, side_of(f)] + bc_in[...]).astype(jnp.bfloat16)
    cross(dt_out, dt_in, 1).wait()
    dt_ref[...] = acc[:, 2 * wide:] + dt_in[...]


def gathered_sums(hidden, shard, wide):
    count = lax.axis_size("seq")
    tokens, total = hidden.shape[0], shard.shape[1]
    f32, bf16 = jnp.float32, jnp.bfloat16
    n = count // 2
    dma = pltpu.SemaphoreType.DMA
    return pl.pallas_call(
        functools.partial(gather_kernel, count),
        out_shape=[jax.ShapeDtypeStruct((tokens, wide), bf16),
                   jax.ShapeDtypeStruct((tokens, total - 2 * wide), f32)],
        in_specs=[VM] * 2,
        out_specs=[VM] * 2,
        scratch_shapes=[
            pltpu.VMEM((count,) + shard.shape, bf16),
            pltpu.VMEM((tokens, total), f32),
            pltpu.VMEM((tokens, wide), f32), pltpu.VMEM((tokens, wide), f32),
            pltpu.VMEM((tokens, total - 2 * wide), f32), pltpu.VMEM((tokens, total - 2 * wide), f32),
            dma((n, PIECES)), dma((n, PIECES)), dma((n, PIECES)), dma((n, PIECES)), dma((2,)), dma((2,)),
        ],
        compiler_params=pltpu.CompilerParams(
            collective_id=1, has_side_effects=True, vmem_limit_bytes=32 * 1024 * 1024),
        cost_estimate=pl.CostEstimate(flops=40_000_000_000, bytes_accessed=40_000_000, transcendentals=0),
        name="gather_project",
    )(hidden, shard)


def body(
    hidden_next, values_next, seg_next, proj_bc, proj_dt, dt_bias, decay_rate, skip_gain,
    bc_prev, dt_prev, seg_prev, grad_prev,
):
    tokens_dev = hidden_next.shape[0]
    bc_width = proj_bc.shape[1]
    heads_all = proj_dt.shape[1]
    fsdp_count = lax.axis_size("fsdp")
    fsdp_place = lax.axis_index("fsdp")
    seq_count = lax.axis_size("seq")
    heads_dev = heads_all // fsdp_count
    state_dim = bc_width // (2 * GW)
    per_group = heads_all // GW
    groups_dev = max(1, heads_dev // per_group)
    first_head = fsdp_place * heads_dev
    first_group = first_head // per_group
    rows_dev = proj_bc.shape[0]
    half = bc_width // 2
    gw = groups_dev * state_dim

    blocks = []
    for f in range(fsdp_count):
        g0 = (f * heads_dev // per_group) * state_dim
        blocks.append([proj_bc[:, g0:g0 + gw], proj_bc[:, half + g0:half + g0 + gw]])
    ring = fsdp_count == 2 and seq_count % 4 == 0 and rows_dev % (2 * LANES) == 0 and heads_all == LANES
    if ring:
        shard = jnp.concatenate([*blocks[0], *blocks[1], proj_dt], axis=1)
        bc_next, dt_sum = gathered_sums(hidden_next, shard, 2 * gw)
        dt_sum = lax.dynamic_slice_in_dim(dt_sum, first_head, heads_dev, 1)
    else:
        pieces = []
        for f in range(fsdp_count):
            pieces += [*blocks[f], proj_dt[:, f * heads_dev:(f + 1) * heads_dev]]
        weights = lax.all_gather(jnp.concatenate(pieces, axis=1), "seq", axis=0, tiled=True)
        owned = lax.dynamic_slice_in_dim(
            hidden_next.reshape(tokens_dev, seq_count, fsdp_count, rows_dev), fsdp_place, 1, 2
        ).reshape(tokens_dev, seq_count * rows_dev)
        sums = lax.psum_scatter(jnp.dot(owned, weights, preferred_element_type=jnp.float32),
                                "fsdp", scatter_dimension=1, tiled=True)
        bc_next, dt_sum = sums[:, :2 * gw].astype(jnp.bfloat16), sums[:, 2 * gw:]

    decay = lax.dynamic_slice_in_dim(decay_rate, first_head, heads_dev, 0)[None]
    skip = lax.dynamic_slice_in_dim(skip_gain, first_head, heads_dev, 0)[None]
    bias = lax.dynamic_slice_in_dim(dt_bias, first_head, heads_dev, 0)[None]

    b_prev = lax.dynamic_slice_in_dim(bc_prev, first_group * state_dim, gw, 1)
    c_prev = lax.dynamic_slice_in_dim(bc_prev, half + first_group * state_dim, gw, 1)
    b_next, c_next = bc_next[:, :gw], bc_next[:, gw:]
    dt_next = jax.nn.softplus(dt_sum + bias)
    out_next, grad_values = chains(
        seg_next, values_next, c_next, b_next, dt_next, decay, skip,
        seg_prev, grad_prev, b_prev, c_prev, dt_prev)
    return (out_next, grad_values)


def solution(mesh):
    in_specs = (
        P("seq", None), P("seq", "fsdp"), P(), P(("seq", "fsdp"), None), P(("seq", "fsdp"), None),
        P(), P(), P(), P("seq", None), P("seq", "fsdp"), P(), P("seq", "fsdp"),
    )
    out_specs = (P("seq", "fsdp"), P("seq", "fsdp"))
    return jax.shard_map(body, mesh=mesh, in_specs=in_specs, out_specs=out_specs, check_vma=False)
```
